32 devices in a mesh: seq: 8 (over z, x), head: 4 (over y, core).
Axes of the slice: x: 2, y: 2, z: 4, core: 2. Of those that a mesh axis runs over, the one named last changes fastest.
Arguments:
- queries: bfloat16 [8192, 2048], P('seq', 'head'), may hold values from -6 to 6
- key_vectors: bfloat16 [8192, 2048], P('seq', 'head'), may hold values from -0.52734375 to 0.52734375
- value_vectors: bfloat16 [8192, 2048], P('seq', 'head'), may hold values from -6 to 6
- out_grad: bfloat16 [8192, 2048], P('seq', 'head'), may hold values from -6 to 6
- head_rates: float32 [16], P('head'), may hold values from 6.1035156e-05 to 0.05
- gate_scale: float32 [16, 8192], P('head', 'seq'), may hold values from 0.5 to 2
Outputs:
- query_gradient: bfloat16 [8192, 2048], P('seq', 'head')
- key_gradient: bfloat16 [8192, 2048], P('seq', 'head')
- value_gradient: bfloat16 [8192, 2048], P('seq', 'head')
The draws below stay inside these ranges and needn't reach their ends.
All inputs are finite; a program needn't handle non-finite values.
Results may differ from the reference program's by a relative error of at most 0.014.
Values may be sent and summed in bfloat16 or wider, within the bound.
A program may use at most 128 MiB of HBM per device.

```python
import math
import jax
import jax.numpy as jnp
from jax import lax

TOK_DEV = 1024
DK = 128
DV = 128
HEADS = 16
LENGTH = 8192


def levels(stream_key, shape, cuts, smallest, top_value):
    factor_of, own = 1.0, jax.random.fold_in(stream_key, 6)
    for axis_at, parts in cuts:
        heights = jnp.exp(jax.random.uniform(jax.random.fold_in(own, axis_at), (parts,), jnp.float32, smallest / len(cuts), top_value / len(cuts)))
        factor_of = factor_of * jnp.repeat(heights, shape[axis_at] // parts).reshape([-1 if axis == axis_at else 1 for axis in range(len(shape))])
    return factor_of


def noise(rng, shape, scale, most, shards=(), kind=jnp.bfloat16):
    result = scale * jax.random.normal(rng, shape, jnp.float32)
    if shards:
        result = result * levels(rng, shape, shards, -0.22, 0.18)
    return jnp.clip(result, -most, most).astype(kind)


def setup_inputs(seed: int = 0) -> dict:
    streams_of = jax.random.split(jax.random.key(seed), 7)
    return {
        "queries": noise(streams_of[0], (LENGTH, HEADS * DK), 1.0, 6.0, ((0, 8), (1, 4))),
        "key_vectors": noise(streams_of[1], (LENGTH, HEADS * DK), (DK ** -0.5), 0.52734375, ((0, 8), (1, 4))),
        "value_vectors": noise(streams_of[2], (LENGTH, HEADS * DV), 1.0, 6.0, ((0, 8), (1, 4))),
        "out_grad": noise(streams_of[3], (LENGTH, HEADS * DV), 1.0, 6.0, ((0, 8), (1, 4))),
        "head_rates": jnp.clip(jnp.exp(math.log(0.05) - 6.7083283 * jax.random.uniform(streams_of[4], (HEADS,), jnp.float32) ** levels(streams_of[4], (HEADS,), ((0, 4),), -0.2, 0.2)), 6.103515625e-05, 0.05),
        "gate_scale": jnp.clip(0.5 + 1.5 * jax.random.uniform(streams_of[5], (HEADS, LENGTH), jnp.float32) ** levels(streams_of[5], (HEADS, LENGTH), ((0, 4), (1, 8)), -0.2, 0.2), 0.5, 2.0),
    }


EPS = 1e-06

def decays(head_rates, gate_block):
    cumulative = jnp.cumsum(-head_rates[:, None] * gate_block, axis=1)
    return (cumulative, cumulative[:, -1])

def causal_factor(cumulative):
    length_here = cumulative.shape[1]
    differences = cumulative[:, :, None] - cumulative[:, None, :]
    lower_mask = jnp.tril(jnp.ones((length_here, length_here), dtype=bool))[None]
    return jnp.where(lower_mask, jnp.exp(jnp.where(lower_mask, differences, 0.0)), 0.0)

def summarize(head_rates, block):
    key_tile_block, value_tile_block, gate_block = block
    cumulative, overall = decays(head_rates, gate_block)
    trailing_portion = jnp.exp(overall[:, None] - cumulative).T[:, :, None]
    damped_key_rows = (key_tile_block.astype(jnp.float32) * trailing_portion).astype(jnp.bfloat16)
    state_increment = jnp.einsum('zun,zui->uni', damped_key_rows.astype(jnp.float32), value_tile_block.astype(jnp.float32))
    return (overall, state_increment)

def recompute(head_rates, block, state):
    query_block, key_tile_block, value_tile_block, grad_block, gate_block = block
    cumulative, overall = decays(head_rates, gate_block)
    head_exponential = jnp.exp(cumulative).T[:, :, None]
    damped_query_rows = (query_block.astype(jnp.float32) * head_exponential).astype(jnp.bfloat16)
    factor = causal_factor(cumulative)
    scores = jnp.einsum('thk,shk->hts', query_block.astype(jnp.float32), key_tile_block.astype(jnp.float32))
    attn_weights = (scores * factor).astype(jnp.bfloat16)
    state_portion = state.astype(jnp.bfloat16)
    output_result = jnp.einsum('gqw,qwx->gqx', damped_query_rows.astype(jnp.float32), state_portion.astype(jnp.float32))
    output_result = output_result + jnp.einsum('hts,shv->thv', attn_weights.astype(jnp.float32), value_tile_block.astype(jnp.float32))
    grad_full = grad_block.astype(jnp.float32)
    square_sum = lax.optimization_barrier(jnp.sum(output_result * output_result, axis=(1, 2)))
    cross_sum = lax.optimization_barrier(jnp.sum(grad_full * output_result, axis=(1, 2)))
    width = HEADS * DV
    root = jnp.sqrt(square_sum / width + EPS)
    output_delta = grad_full / root[:, None, None] - output_result * (cross_sum / (width * root ** 3))[:, None, None]
    output_delta = output_delta.astype(jnp.bfloat16)
    return (cumulative, overall, damped_query_rows, factor, attn_weights, output_delta)

def gradients(block, cumulative, overall, factor, attn_weights, output_delta, state, later):
    query_block = block[0].astype(jnp.float32)
    key_tile_block = block[1].astype(jnp.float32)
    value_tile_block = block[2].astype(jnp.float32)
    complete_output_delta = output_delta.astype(jnp.float32)
    mixed = jnp.einsum('thv,shv->hts', complete_output_delta, value_tile_block) * factor
    mixed_half = mixed.astype(jnp.bfloat16).astype(jnp.float32)
    state_portion = state.astype(jnp.bfloat16).astype(jnp.float32)
    second_portion = later.astype(jnp.bfloat16).astype(jnp.float32)
    head_exponential = jnp.exp(cumulative).T[:, :, None]
    trailing_portion = jnp.exp(overall[:, None] - cumulative).T[:, :, None]
    query_gradient = head_exponential * jnp.einsum('syi,ybi->syb', complete_output_delta, state_portion)
    query_gradient = query_gradient + jnp.einsum('hts,shk->thk', mixed_half, key_tile_block)
    key_gradient = trailing_portion * jnp.einsum('zxl,xfl->zxf', value_tile_block, second_portion)
    key_gradient = key_gradient + jnp.einsum('hts,thk->shk', mixed_half, query_block)
    value_gradient = trailing_portion * jnp.einsum('jip,ipa->jia', key_tile_block, second_portion)
    value_gradient = value_gradient + jnp.einsum('hts,thv->shv', attn_weights.astype(jnp.float32), complete_output_delta)
    return (query_gradient.astype(jnp.bfloat16), key_gradient.astype(jnp.bfloat16), value_gradient.astype(jnp.bfloat16))

def reference(queries, key_vectors, value_vectors, out_grad, head_rates, gate_scale):
    blocks = LENGTH // TOK_DEV

    def split_rows(array, depth):
        return array.reshape(blocks, TOK_DEV, HEADS, depth)
    query_blocks = split_rows(queries, DK)
    key_blocks = split_rows(key_vectors, DK)
    value_blocks = split_rows(value_vectors, DV)
    grad_blocks = split_rows(out_grad, DV)
    gate_blocks = gate_scale.reshape(HEADS, blocks, TOK_DEV).transpose(1, 0, 2)
    overall_all, updates = lax.map(lambda item: summarize(head_rates, item), (key_blocks, value_blocks, gate_blocks))
    start_state = jnp.zeros((HEADS, DK, DV), jnp.float32)

    def forward(state, item):
        return (jnp.exp(item[0])[:, None, None] * state + item[1], state)
    _, leading_portion = lax.scan(forward, start_state, (overall_all, updates))
    inputs = (query_blocks, key_blocks, value_blocks, grad_blocks, gate_blocks)

    def middle(item):
        portion_list = recompute(head_rates, item[:5], item[5])
        return jnp.einsum('zun,zui->uni', portion_list[2].astype(jnp.float32), portion_list[5].astype(jnp.float32))
    grad_sums = lax.map(middle, inputs + (leading_portion,))

    def backward(state, item):
        return (item[1] + jnp.exp(item[0])[:, None, None] * state, state)
    _, suffix = lax.scan(backward, start_state, (overall_all, grad_sums), reverse=True)

    def final(item):
        cumulative, overall, damped_query_rows, factor, attn_weights, output_delta = recompute(head_rates, item[:5], item[5])
        return gradients(item[:5], cumulative, overall, factor, attn_weights, output_delta, item[5], item[6])
    query_gradient, key_gradient, value_gradient = lax.map(final, inputs + (leading_portion, suffix))
    return (query_gradient.reshape(LENGTH, HEADS * DK), key_gradient.reshape(LENGTH, HEADS * DK), value_gradient.reshape(LENGTH, HEADS * DV))
```

```python
import functools

import jax
import jax.numpy as jnp
from jax import lax
from jax.experimental import pallas as pl
from jax.experimental.pallas import tpu as pltpu
from jax.sharding import PartitionSpec as P

EPS = 1e-06
F32 = jnp.float32
BF16 = jnp.bfloat16
MESH = pl.DeviceIdType.MESH


def dot(a, b, ca, cb, **kw):
    return lax.dot_general(
        a, b, (((ca,), (cb,)), ((), ())), preferred_element_type=F32, **kw
    )


def kernel(
    n, nh, H, T, D, C,
    rates, gate, q_hbm, k_hbm, v_hbm, g_hbm,
    dq_out, dk_out, dv_out,
    q, k, v, g, lrep, brow, bc, gown, gpeer,
    sl, w, o, macc, xacc, pstate, pchunk, sp,
    ubuf, upeer, cin, cout, stat, statin, tr,
    dob, vbuf, vpeer, din, dout, rl, dk1, dv1,
    in_sem, g_sem, us, ur, cs, cr, ss, sr, vs, vr, ds, dr,
):
    J = T // C
    LAST = n // 2 - 1
    me = lax.axis_index("seq")
    hd = lax.axis_index("head")
    inner = lax.rem(me, 2)
    z = me // 2
    peer = me + 1 - 2 * inner
    nxt = lax.rem(me + 2, n)
    prv = lax.rem(me + n - 2, n)

    def cols(h):
        start = h * D
        if not isinstance(h, int):
            start = pl.multiple_of(start, D)
        return pl.ds(start, D)

    def load(i, src, dst, h):
        return pltpu.make_async_copy(
            src.at[:, cols(h)], dst.at[:, cols(h)], in_sem.at[i, h]
        )

    for i, (src, dst) in enumerate(((k_hbm, k), (v_hbm, v), (q_hbm, q), (g_hbm, g))):
        for h in range(H):
            load(i, src, dst, h).start()

    barrier = pltpu.get_barrier_semaphore()
    for s in (peer, nxt, prv):
        pl.semaphore_signal(barrier, inc=1, device_id={"seq": s}, device_id_type=MESH)
    for d in range(1, nh):
        pl.semaphore_signal(
            barrier, inc=1, device_id={"head": lax.rem(hd + d, nh)}, device_id_type=MESH
        )

    def remote(src, dst, s_sem, r_sem, **to):
        return pltpu.make_async_remote_copy(
            src_ref=src, dst_ref=dst, send_sem=s_sem, recv_sem=r_sem,
            device_id=to, device_id_type=MESH,
        )

    l = -rates[...] * gate[...]
    for i in range(128 // H):
        lrep[i * H:(i + 1) * H, :] = l
    ri = lax.broadcasted_iota(jnp.int32, (C, C), 0)
    ci = lax.broadcasted_iota(jnp.int32, (C, C), 1)
    triu = jnp.where(ri <= ci, 1.0, 0.0).astype(F32)
    tot = [None] * H
    for j in range(J):
        r = dot(lrep[:, j * C:(j + 1) * C], triu, 1, 0, precision=lax.Precision.HIGHEST)
        brow[j] = r[0:8, :]
        col = r.T
        for h in range(H):
            b = jnp.broadcast_to(col[:, h:h + 1], (C, D))
            bc[h, j * C:(j + 1) * C, :] = b
            e = b[C - 1:C, :]
            tot[h] = e if tot[h] is None else tot[h] + e
    for h in range(H):
        gown[h:h + 1, :] = tot[h]

    gown[H:8, :] = jnp.zeros((8 - H, D), F32)
    pl.semaphore_wait(barrier, 3 + nh - 1)
    gcopy = remote(gown, gpeer, g_sem.at[0], g_sem.at[1], seq=peer)
    gcopy.start()

    def ucopy(h):
        return remote(ubuf.at[h], upeer.at[h], us.at[h], ur.at[h], seq=peer)

    def ccopy(h):
        return remote(cout.at[h], cin.at[h], cs.at[h], cr.at[h], seq=nxt)

    def vcopy(h):
        return remote(vbuf.at[h], vpeer.at[h], vs.at[h], vr.at[h], seq=peer)

    def dcopy(h):
        return remote(dout.at[h], din.at[h], ds.at[h], dr.at[h], seq=prv)

    def loop(lo, hi, fn):
        def step(h, carry):
            fn(h)
            return carry
        lax.fori_loop(lo, hi, step, 0)

    def rows(j):
        return slice(j * C, (j + 1) * C)

    def updates(h):
        load(0, k_hbm, k, h).wait()
        load(1, v_hbm, v, h).wait()
        s = jnp.zeros((D, D), F32)
        for j in range(J):
            b = bc[h, rows(j), :]
            e = b[C - 1:C, :]
            kd = (k[rows(j), cols(h)].astype(F32) * jnp.exp(e - b)).astype(BF16)
            u = dot(kd, v[rows(j), cols(h)], 0, 0)
            sl[h * (J + 1) + j] = s
            s = u if j == 0 else jnp.exp(e) * s + u
        sl[h * (J + 1) + J] = s
        ubuf[h] = s.astype(BF16)
        ucopy(h).start()

    loop(0, H, updates)

    def factor(h, j):
        b = bc[h, rows(j), :]
        left = jnp.concatenate([b] * (C // D), axis=1)
        right = brow[j, pl.ds(h, 1), :]
        return jnp.exp(jnp.where(ri >= ci, left - right, -jnp.inf))

    def intra(h):
        load(2, q_hbm, q, h).wait()
        for j in range(J):
            wj = dot(q[rows(j), cols(h)], k[rows(j), cols(h)], 1, 1) * factor(h, j)
            wj = wj.astype(BF16)
            w[h * J + j] = wj
            o[rows(j), cols(h)] = dot(wj, v[rows(j), cols(h)], 1, 0)

    half = H // 2
    loop(0, half, intra)
    gcopy.wait()

    def ex(ref, h):
        return jnp.exp(ref[pl.ds(h, 1), :])

    def pair(h):
        ucopy(h).wait_recv()
        own = sl[h * (J + 1) + J]

        @pl.when(inner == 0)
        def _():
            sp[h] = ex(gpeer, h) * own + upeer[h].astype(F32)

        @pl.when(inner == 1)
        def _():
            sp[h] = ex(gown, h) * upeer[h].astype(F32) + own

        @pl.when(z == 0)
        def _():
            cout[h] = sp[h].astype(BF16)
            cin[h] = jnp.zeros((D, D), BF16)

            @pl.when(z < LAST)
            def _():
                ccopy(h).start()

    loop(0, H, pair)
    loop(half, H, intra)
    for h in range(H):
        load(3, g_hbm, g, h).wait()

    def chain(h):
        @pl.when(z > 0)
        def _():
            ccopy(h).wait_recv()

            @pl.when(z < LAST)
            def _():
                a = ex(gown, h) * ex(gpeer, h)
                cout[h] = (a * cin[h].astype(F32) + sp[h]).astype(BF16)
                ccopy(h).start()

        @pl.when(inner == 0)
        def _():
            pstate[h] = cin[h].astype(F32)

        @pl.when(inner == 1)
        def _():
            pstate[h] = ex(gpeer, h) * cin[h].astype(F32) + upeer[h].astype(F32)

        s = pstate[h]
        for j in range(J):
            pj = (s + sl[h * (J + 1) + j] if j else s).astype(BF16)
            pchunk[h * J + j] = pj
            b = bc[h, rows(j), :]
            s = s * jnp.exp(b[C - 1:C, :])
            qe = (q[rows(j), cols(h)].astype(F32) * jnp.exp(b)).astype(BF16)
            oj = o[rows(j), cols(h)] + dot(qe, pj, 1, 0)
            o[rows(j), cols(h)] = oj
            gj = g[rows(j), cols(h)].astype(F32)

            @pl.when(h == 0)
            def _():
                macc[rows(j), :] = oj * oj
                xacc[rows(j), :] = gj * oj

            @pl.when(h > 0)
            def _():
                macc[rows(j), :] += oj * oj
                xacc[rows(j), :] += gj * oj

    loop(0, H, chain)

    NG = T // 128
    lane = lax.broadcasted_iota(jnp.int32, (128, 128), 1)
    acc = jnp.zeros((128, 128), F32)
    for u in range(NG):
        part = slice(u * 128, (u + 1) * 128)
        acc = jnp.where(lane == u, jnp.sum(macc[part, :], axis=1, keepdims=True), acc)
        acc = jnp.where(lane == NG + u, jnp.sum(xacc[part, :], axis=1, keepdims=True), acc)
    stat[...] = acc.T[0:2 * NG, :]
    scopies = [
        remote(stat, statin.at[d - 1], ss.at[d - 1], sr.at[d - 1], head=lax.rem(hd + d, nh))
        for d in range(1, nh)
    ]
    for c in scopies:
        c.start()
    for c in scopies:
        c.wait_recv()
    whole = stat[...]
    for d in range(nh - 1):
        whole = whole + statin[d]
    width = float(H * nh * D)
    root = jnp.sqrt(whole[0:NG] / width + EPS)
    tr[...] = jnp.zeros_like(tr)
    tr[0:NG, :] = 1.0 / root
    tr[NG:2 * NG, :] = whole[NG:2 * NG] / (width * root * root * root)
    back = tr[...].T
    for u in range(NG):
        part = slice(u * 128, (u + 1) * 128)
        macc[part, :] = jnp.broadcast_to(back[:, u:u + 1], (128, D))
        xacc[part, :] = jnp.broadcast_to(back[:, NG + u:NG + u + 1], (128, D))

    def outgrad(h):
        s = None
        for j in reversed(range(J)):
            do = (
                g[rows(j), cols(h)].astype(F32) * macc[rows(j), :]
                - o[rows(j), cols(h)] * xacc[rows(j), :]
            ).astype(BF16)
            dob[rows(j), cols(h)] = do
            b = bc[h, rows(j), :]
            qe = (q[rows(j), cols(h)].astype(F32) * jnp.exp(b)).astype(BF16)
            u = dot(qe, do, 0, 0)
            rl[h * (J + 1) + j + 1] = jnp.zeros((D, D), F32) if s is None else s
            s = u if s is None else u + jnp.exp(b[C - 1:C, :]) * s
        rl[h * (J + 1)] = s
        vbuf[h] = s.astype(BF16)
        vcopy(h).start()

    loop(0, H, outgrad)

    def grads(h):
        for j in range(J):
            do = dob[rows(j), cols(h)]
            e = (dot(do, v[rows(j), cols(h)], 1, 1) * factor(h, j)).astype(BF16)
            eb = jnp.exp(bc[h, rows(j), :])
            dq_out[rows(j), cols(h)] = (
                eb * dot(do, pchunk[h * J + j], 1, 1) + dot(e, k[rows(j), cols(h)], 1, 0)
            ).astype(BF16)
            dk1[rows(j), cols(h)] = dot(e, q[rows(j), cols(h)], 0, 0)
            dv1[rows(j), cols(h)] = dot(w[h * J + j], do, 0, 0)

    loop(0, half, grads)

    def pair_back(h):
        vcopy(h).wait_recv()
        own = rl[h * (J + 1)]

        @pl.when(inner == 0)
        def _():
            sp[h] = own + ex(gown, h) * vpeer[h].astype(F32)

        @pl.when(inner == 1)
        def _():
            sp[h] = vpeer[h].astype(F32) + ex(gpeer, h) * own

        @pl.when(z == LAST)
        def _():
            dout[h] = sp[h].astype(BF16)
            din[h] = jnp.zeros((D, D), BF16)

            @pl.when(z > 0)
            def _():
                dcopy(h).start()

    loop(0, H, pair_back)
    loop(half, H, grads)

    def chain_back(h):
        @pl.when(z < LAST)
        def _():
            dcopy(h).wait_recv()

            @pl.when(z > 0)
            def _():
                a = ex(gown, h) * ex(gpeer, h)
                dout[h] = (a * din[h].astype(F32) + sp[h]).astype(BF16)
                dcopy(h).start()

        @pl.when(inner == 1)
        def _():
            pstate[h] = din[h].astype(F32)

        @pl.when(inner == 0)
        def _():
            pstate[h] = ex(gpeer, h) * din[h].astype(F32) + vpeer[h].astype(F32)

        s = pstate[h]
        for j in reversed(range(J)):
            rj = (s + rl[h * (J + 1) + j + 1] if j < J - 1 else s).astype(BF16)
            b = bc[h, rows(j), :]
            e = b[C - 1:C, :]
            s = s * jnp.exp(e)
            tail = jnp.exp(e - b)
            dk_out[rows(j), cols(h)] = (
                dk1[rows(j), cols(h)] + tail * dot(v[rows(j), cols(h)], rj, 1, 1)
            ).astype(BF16)
            dv_out[rows(j), cols(h)] = (
                dv1[rows(j), cols(h)] + tail * dot(k[rows(j), cols(h)], rj, 1, 0)
            ).astype(BF16)

    loop(0, H, chain_back)

    for c in scopies:
        c.wait_send()

    def drain(h):
        ucopy(h).wait_send()
        vcopy(h).wait_send()

        @pl.when(z < LAST)
        def _():
            ccopy(h).wait_send()

        @pl.when(z > 0)
        def _():
            dcopy(h).wait_send()

    loop(0, H, drain)


def body(queries, key_vectors, value_vectors, out_grad, head_rates, gate_scale):
    H, T = gate_scale.shape
    D = queries.shape[1] // H
    n = lax.axis_size("seq")
    nh = lax.axis_size("head")
    C = min(256, T)
    J = T // C
    tile = pltpu.VMEM((H, D, D), BF16)
    full = pltpu.VMEM((T, H * D), BF16)
    wide = pltpu.VMEM((T, H * D), F32)
    sem = pltpu.SemaphoreType.DMA
    out = jax.ShapeDtypeStruct((T, H * D), BF16)
    vm = pl.BlockSpec(memory_space=pltpu.VMEM)
    hbm = pl.BlockSpec(memory_space=pl.ANY)
    return pl.pallas_call(
        functools.partial(kernel, n, nh, H, T, D, C),
        out_shape=(out, out, out),
        in_specs=[vm, vm, hbm, hbm, hbm, hbm],
        out_specs=(vm, vm, vm),
        scratch_shapes=[
            full, full, full, full,
            pltpu.VMEM((128, T), F32),
            pltpu.VMEM((J, 8, C), F32),
            pltpu.VMEM((H, T, D), F32),
            pltpu.VMEM((8, D), F32),
            pltpu.VMEM((8, D), F32),
            pltpu.VMEM((H * (J + 1), D, D), F32),
            pltpu.VMEM((H * J, C, C), BF16),
            wide,
            pltpu.VMEM((T, D), F32),
            pltpu.VMEM((T, D), F32),
            pltpu.VMEM((H, D, D), F32),
            pltpu.VMEM((H * J, D, D), BF16),
            pltpu.VMEM((H, D, D), F32),
            tile, tile, tile, tile,
            pltpu.VMEM((2 * T // 128, 128), F32),
            pltpu.VMEM((nh - 1, 2 * T // 128, 128), F32),
            pltpu.VMEM((128, 128), F32),
            full,
            tile, tile, tile, tile,
            pltpu.VMEM((H * (J + 1), D, D), F32),
            wide, wide,
            sem((4, H)), sem((2,)),
            sem((H,)), sem((H,)), sem((H,)), sem((H,)),
            sem((nh - 1,)), sem((nh - 1,)),
            sem((H,)), sem((H,)), sem((H,)), sem((H,)),
        ],
        compiler_params=pltpu.CompilerParams(
            collective_id=0, has_side_effects=True, vmem_limit_bytes=44 * 1024 * 1024
        ),
    )(head_rates[:, None], gate_scale, queries, key_vectors, value_vectors, out_grad)


def solution(mesh):
    placed = (
        P("seq", "head"),
        P("seq", "head"),
        P("seq", "head"),
        P("seq", "head"),
        P("head"),
        P("head", "seq"),
    )
    return jax.shard_map(
        body,
        mesh=mesh,
        in_specs=placed,
        out_specs=(P("seq", "head"), P("seq", "head"), P("seq", "head")),
        check_vma=False,
    )
```

```python
import functools

import jax
import jax.numpy as jnp
from jax import lax
from jax.experimental import pallas as pl
from jax.experimental.pallas import tpu as pltpu
from jax.sharding import PartitionSpec as P

EPS = 1e-06
F32 = jnp.float32
BF16 = jnp.bfloat16
MESH = pl.DeviceIdType.MESH


def dot(a, b, ca, cb, **kw):
    return lax.dot_general(
        a, b, (((ca,), (cb,)), ((), ())), preferred_element_type=F32, **kw
    )


def kernel(
    n, nh, H, T, D, C,
    rates, gate_hbm, q_hbm, k_hbm, v_hbm, g_hbm,
    dq_out, dk_out, dv_out,
    gate, q, k, v, g, lrep, brow, bc, gown, gpeer,
    sl, w, o, macc, xacc, pstate, pchunk, sp,
    ubuf, upeer, cin, cout, stat, statin, tr,
    dob, vbuf, vpeer, din, dout, rl, dk1, dv1,
    in_sem, gate_sem, g_sem, us, ur, cs, cr, ss, sr, vs, vr, ds, dr,
):
    J = T // C
    LAST = n // 2 - 1
    me = lax.axis_index("seq")
    hd = lax.axis_index("head")
    inner = lax.rem(me, 2)
    z = me // 2
    peer = me + 1 - 2 * inner
    nxt = lax.rem(me + 2, n)
    prv = lax.rem(me + n - 2, n)

    def cols(h):
        start = h * D
        if not isinstance(h, int):
            start = pl.multiple_of(start, D)
        return pl.ds(start, D)

    def load(i, src, dst, h):
        return pltpu.make_async_copy(
            src.at[:, cols(h)], dst.at[:, cols(h)], in_sem.at[i, h]
        )

    gate_copy = pltpu.make_async_copy(gate_hbm, gate, gate_sem.at[0])
    gate_copy.start()
    for i, (src, dst) in enumerate(((k_hbm, k), (v_hbm, v), (q_hbm, q), (g_hbm, g))):
        for h in range(H):
            load(i, src, dst, h).start()

    barrier = pltpu.get_barrier_semaphore()
    for s in (peer, nxt, prv):
        pl.semaphore_signal(barrier, inc=1, device_id={"seq": s}, device_id_type=MESH)
    for d in range(1, nh):
        pl.semaphore_signal(
            barrier, inc=1, device_id={"head": lax.rem(hd + d, nh)}, device_id_type=MESH
        )

    def remote(src, dst, s_sem, r_sem, **to):
        return pltpu.make_async_remote_copy(
            src_ref=src, dst_ref=dst, send_sem=s_sem, recv_sem=r_sem,
            device_id=to, device_id_type=MESH,
        )

    gate_copy.wait()
    l = jnp.concatenate([gate[h:h + 1, :] * -rates[h] for h in range(H)], axis=0)
    for i in range(128 // H):
        lrep[i * H:(i + 1) * H, :] = l
    ri = lax.broadcasted_iota(jnp.int32, (C, C), 0)
    ci = lax.broadcasted_iota(jnp.int32, (C, C), 1)
    triu = jnp.where(ri <= ci, 1.0, 0.0).astype(BF16)
    tot = [None] * H
    for j in range(J):
        lj = lrep[:, j * C:(j + 1) * C]
        hi = lj.astype(BF16)
        rest = lj - hi.astype(F32)
        mid = rest.astype(BF16)
        low = (rest - mid.astype(F32)).astype(BF16)
        r = dot(low, triu, 1, 0) + dot(mid, triu, 1, 0) + dot(hi, triu, 1, 0)
        brow[j] = r[0:8, :]
        col = r.T
        for h in range(H):
            b = jnp.broadcast_to(col[:, h:h + 1], (C, D))
            bc[h, j * C:(j + 1) * C, :] = b
            e = b[C - 1:C, :]
            tot[h] = e if tot[h] is None else tot[h] + e
    for h in range(H):
        gown[h:h + 1, :] = tot[h]

    gown[H:8, :] = jnp.zeros((8 - H, D), F32)
    pl.semaphore_wait(barrier, 3 + nh - 1)
    gcopy = remote(gown, gpeer, g_sem.at[0], g_sem.at[1], seq=peer)
    gcopy.start()

    def ucopy(h):
        return remote(ubuf.at[h], upeer.at[h], us.at[h], ur.at[h], seq=peer)

    def ccopy(h):
        return remote(cout.at[h], cin.at[h], cs.at[h], cr.at[h], seq=nxt)

    def vcopy(h):
        return remote(vbuf.at[h], vpeer.at[h], vs.at[h], vr.at[h], seq=peer)

    def dcopy(h):
        return remote(dout.at[h], din.at[h], ds.at[h], dr.at[h], seq=prv)

    def loop(lo, hi, fn):
        def step(h, carry):
            fn(h)
            return carry
        lax.fori_loop(lo, hi, step, 0)

    def rows(j):
        return slice(j * C, (j + 1) * C)

    def updates(h):
        load(0, k_hbm, k, h).wait()
        load(1, v_hbm, v, h).wait()
        s = jnp.zeros((D, D), F32)
        for j in range(J):
            b = bc[h, rows(j), :]
            e = b[C - 1:C, :]
            kd = (k[rows(j), cols(h)].astype(F32) * jnp.exp(e - b)).astype(BF16)
            u = dot(kd, v[rows(j), cols(h)], 0, 0)
            sl[h * (J + 1) + j] = s
            s = u if j == 0 else jnp.exp(e) * s + u
        sl[h * (J + 1) + J] = s
        ubuf[h] = s.astype(BF16)
        ucopy(h).start()

    loop(0, H, updates)

    def factor(h, j):
        b = bc[h, rows(j), :]
        left = jnp.concatenate([b] * (C // D), axis=1)
        right = brow[j, pl.ds(h, 1), :]
        return jnp.exp(jnp.where(ri >= ci, left - right, -jnp.inf))

    def intra(h):
        load(2, q_hbm, q, h).wait()
        for j in range(J):
            wj = dot(q[rows(j), cols(h)], k[rows(j), cols(h)], 1, 1) * factor(h, j)
            wj = wj.astype(BF16)
            w[h * J + j] = wj
            o[rows(j), cols(h)] = dot(wj, v[rows(j), cols(h)], 1, 0)

    half = H // 2
    loop(0, half, intra)
    gcopy.wait()

    def ex(ref, h):
        return jnp.exp(ref[pl.ds(h, 1), :])

    def pair(h):
        ucopy(h).wait_recv()
        own = sl[h * (J + 1) + J]

        @pl.when(inner == 0)
        def _():
            sp[h] = ex(gpeer, h) * own + upeer[h].astype(F32)

        @pl.when(inner == 1)
        def _():
            sp[h] = ex(gown, h) * upeer[h].astype(F32) + own

        @pl.when(z == 0)
        def _():
            cout[h] = sp[h].astype(BF16)
            cin[h] = jnp.zeros((D, D), BF16)

            @pl.when(z < LAST)
            def _():
                ccopy(h).start()

    loop(0, H, pair)
    loop(half, H, intra)
    for h in range(H):
        load(3, g_hbm, g, h).wait()

    def chain(h):
        @pl.when(z > 0)
        def _():
            ccopy(h).wait_recv()

            @pl.when(z < LAST)
            def _():
                a = ex(gown, h) * ex(gpeer, h)
                cout[h] = (a * cin[h].astype(F32) + sp[h]).astype(BF16)
                ccopy(h).start()

        @pl.when(inner == 0)
        def _():
            pstate[h] = cin[h].astype(F32)

        @pl.when(inner == 1)
        def _():
            pstate[h] = ex(gpeer, h) * cin[h].astype(F32) + upeer[h].astype(F32)

        s = pstate[h]
        for j in range(J):
            pj = (s + sl[h * (J + 1) + j] if j else s).astype(BF16)
            pchunk[h * J + j] = pj
            b = bc[h, rows(j), :]
            s = s * jnp.exp(b[C - 1:C, :])
            qe = (q[rows(j), cols(h)].astype(F32) * jnp.exp(b)).astype(BF16)
            oj = o[rows(j), cols(h)] + dot(qe, pj, 1, 0)
            o[rows(j), cols(h)] = oj
            gj = g[rows(j), cols(h)].astype(F32)

            @pl.when(h == 0)
            def _():
                macc[rows(j), :] = oj * oj
                xacc[rows(j), :] = gj * oj

            @pl.when(h > 0)
            def _():
                macc[rows(j), :] += oj * oj
                xacc[rows(j), :] += gj * oj

    loop(0, H, chain)

    NG = T // 128
    lane = lax.broadcasted_iota(jnp.int32, (128, 128), 1)
    acc = jnp.zeros((128, 128), F32)
    for u in range(NG):
        part = slice(u * 128, (u + 1) * 128)
        acc = jnp.where(lane == u, jnp.sum(macc[part, :], axis=1, keepdims=True), acc)
        acc = jnp.where(lane == NG + u, jnp.sum(xacc[part, :], axis=1, keepdims=True), acc)
    stat[...] = acc.T[0:2 * NG, :]
    scopies = [
        remote(stat, statin.at[d - 1], ss.at[d - 1], sr.at[d - 1], head=lax.rem(hd + d, nh))
        for d in range(1, nh)
    ]
    for c in scopies:
        c.start()
    for c in scopies:
        c.wait_recv()
    whole = stat[...]
    for d in range(nh - 1):
        whole = whole + statin[d]
    width = float(H * nh * D)
    root = jnp.sqrt(whole[0:NG] / width + EPS)
    tr[...] = jnp.zeros_like(tr)
    tr[0:NG, :] = 1.0 / root
    tr[NG:2 * NG, :] = whole[NG:2 * NG] / (width * root * root * root)
    back = tr[...].T
    for u in range(NG):
        part = slice(u * 128, (u + 1) * 128)
        macc[part, :] = jnp.broadcast_to(back[:, u:u + 1], (128, D))
        xacc[part, :] = jnp.broadcast_to(back[:, NG + u:NG + u + 1], (128, D))

    def outgrad(h):
        s = None
        for j in reversed(range(J)):
            do = (
                g[rows(j), cols(h)].astype(F32) * macc[rows(j), :]
                - o[rows(j), cols(h)] * xacc[rows(j), :]
            ).astype(BF16)
            dob[rows(j), cols(h)] = do
            b = bc[h, rows(j), :]
            qe = (q[rows(j), cols(h)].astype(F32) * jnp.exp(b)).astype(BF16)
            u = dot(qe, do, 0, 0)
            rl[h * (J + 1) + j + 1] = jnp.zeros((D, D), F32) if s is None else s
            s = u if s is None else u + jnp.exp(b[C - 1:C, :]) * s
        rl[h * (J + 1)] = s
        vbuf[h] = s.astype(BF16)
        vcopy(h).start()

    loop(0, H, outgrad)

    def grads(h):
        for j in range(J):
            do = dob[rows(j), cols(h)]
            e = (dot(do, v[rows(j), cols(h)], 1, 1) * factor(h, j)).astype(BF16)
            eb = jnp.exp(bc[h, rows(j), :])
            dq_out[rows(j), cols(h)] = (
                eb * dot(do, pchunk[h * J + j], 1, 1) + dot(e, k[rows(j), cols(h)], 1, 0)
            ).astype(BF16)
            dk1[rows(j), cols(h)] = dot(e, q[rows(j), cols(h)], 0, 0)
            dv1[rows(j), cols(h)] = dot(w[h * J + j], do, 0, 0)

    loop(0, half, grads)

    def pair_back(h):
        vcopy(h).wait_recv()
        own = rl[h * (J + 1)]

        @pl.when(inner == 0)
        def _():
            sp[h] = own + ex(gown, h) * vpeer[h].astype(F32)

        @pl.when(inner == 1)
        def _():
            sp[h] = vpeer[h].astype(F32) + ex(gpeer, h) * own

        @pl.when(z == LAST)
        def _():
            dout[h] = sp[h].astype(BF16)
            din[h] = jnp.zeros((D, D), BF16)

            @pl.when(z > 0)
            def _():
                dcopy(h).start()

    loop(0, H, pair_back)
    loop(half, H, grads)

    def chain_back(h):
        @pl.when(z < LAST)
        def _():
            dcopy(h).wait_recv()

            @pl.when(z > 0)
            def _():
                a = ex(gown, h) * ex(gpeer, h)
                dout[h] = (a * din[h].astype(F32) + sp[h]).astype(BF16)
                dcopy(h).start()

        @pl.when(inner == 1)
        def _():
            pstate[h] = din[h].astype(F32)

        @pl.when(inner == 0)
        def _():
            pstate[h] = ex(gpeer, h) * din[h].astype(F32) + vpeer[h].astype(F32)

        s = pstate[h]
        for j in reversed(range(J)):
            rj = (s + rl[h * (J + 1) + j + 1] if j < J - 1 else s).astype(BF16)
            b = bc[h, rows(j), :]
            e = b[C - 1:C, :]
            s = s * jnp.exp(e)
            tail = jnp.exp(e - b)
            dk_out[rows(j), cols(h)] = (
                dk1[rows(j), cols(h)] + tail * dot(v[rows(j), cols(h)], rj, 1, 1)
            ).astype(BF16)
            dv_out[rows(j), cols(h)] = (
                dv1[rows(j), cols(h)] + tail * dot(k[rows(j), cols(h)], rj, 1, 0)
            ).astype(BF16)

    loop(0, H, chain_back)

    for c in scopies:
        c.wait_send()

    def drain(h):
        ucopy(h).wait_send()
        vcopy(h).wait_send()

        @pl.when(z < LAST)
        def _():
            ccopy(h).wait_send()

        @pl.when(z > 0)
        def _():
            dcopy(h).wait_send()

    loop(0, H, drain)


def body(queries, key_vectors, value_vectors, out_grad, head_rates, gate_scale):
    H, T = gate_scale.shape
    D = queries.shape[1] // H
    n = lax.axis_size("seq")
    nh = lax.axis_size("head")
    C = min(256, T)
    J = T // C
    tile = pltpu.VMEM((H, D, D), BF16)
    full = pltpu.VMEM((T, H * D), BF16)
    wide = pltpu.VMEM((T, H * D), F32)
    sem = pltpu.SemaphoreType.DMA
    out = pltpu.VMEM((T, H * D), BF16)
    vm = pl.BlockSpec(memory_space=pltpu.VMEM)
    hbm = pl.BlockSpec(memory_space=pl.ANY)
    return pl.pallas_call(
        functools.partial(kernel, n, nh, H, T, D, C),
        out_shape=(out, out, out),
        in_specs=[pl.BlockSpec(memory_space=pltpu.SMEM), hbm, hbm, hbm, hbm, hbm],
        out_specs=(vm, vm, vm),
        scratch_shapes=[
            pltpu.VMEM((H, T), F32),
            full, full, full, full,
            pltpu.VMEM((128, T), F32),
            pltpu.VMEM((J, 8, C), F32),
            pltpu.VMEM((H, T, D), F32),
            pltpu.VMEM((8, D), F32),
            pltpu.VMEM((8, D), F32),
            pltpu.VMEM((H * (J + 1), D, D), F32),
            pltpu.VMEM((H * J, C, C), BF16),
            wide,
            pltpu.VMEM((T, D), F32),
            pltpu.VMEM((T, D), F32),
            pltpu.VMEM((H, D, D), F32),
            pltpu.VMEM((H * J, D, D), BF16),
            pltpu.VMEM((H, D, D), F32),
            tile, tile, tile, tile,
            pltpu.VMEM((2 * T // 128, 128), F32),
            pltpu.VMEM((nh - 1, 2 * T // 128, 128), F32),
            pltpu.VMEM((128, 128), F32),
            full,
            tile, tile, tile, tile,
            pltpu.VMEM((H * (J + 1), D, D), F32),
            wide, wide,
            sem((4, H)), sem((1,)), sem((2,)),
            sem((H,)), sem((H,)), sem((H,)), sem((H,)),
            sem((nh - 1,)), sem((nh - 1,)),
            sem((H,)), sem((H,)), sem((H,)), sem((H,)),
        ],
        compiler_params=pltpu.CompilerParams(
            collective_id=0, has_side_effects=True, vmem_limit_bytes=63692800
        ),
    )(head_rates, gate_scale, queries, key_vectors, value_vectors, out_grad)


def solution(mesh):
    placed = (
        P("seq", "head"),
        P("seq", "head"),
        P("seq", "head"),
        P("seq", "head"),
        P("head"),
        P("head", "seq"),
    )
    return jax.shard_map(
        body,
        mesh=mesh,
        in_specs=placed,
        out_specs=(P("seq", "head"), P("seq", "head"), P("seq", "head")),
        check_vma=False,
    )
```

```python
import functools

import jax
import jax.numpy as jnp
from jax import lax
from jax.experimental import pallas as pl
from jax.experimental.pallas import tpu as pltpu
from jax.sharding import PartitionSpec as P

EPS = 1e-06
F32 = jnp.float32
BF16 = jnp.bfloat16
MESH = pl.DeviceIdType.MESH


def dot(a, b, ca, cb, **kw):
    return lax.dot_general(
        a, b, (((ca,), (cb,)), ((), ())), preferred_element_type=F32, **kw
    )


def kernel(
    n, nh, H, T, D, C,
    rates, gate_hbm, q_hbm, k_hbm, v_hbm, g_hbm,
    dq_out, dk_out, dv_out,
    gate, q, k, v, g, lrep, brow, bc, gown, gpeer,
    sl, w, o, macc, xacc, pstate, pchunk, sp,
    ubuf, upeer, cin, cout, stat, statin, tr,
    dob, vbuf, vpeer, din, dout, rl, dk1, dv1,
    in_sem, gate_sem, g_sem, us, ur, cs, cr, ss, sr, vs, vr, ds, dr,
):
    J = T // C
    LAST = n // 2 - 1
    me = lax.axis_index("seq")
    hd = lax.axis_index("head")
    inner = lax.rem(me, 2)
    z = me // 2
    peer = me + 1 - 2 * inner
    nxt = lax.rem(me + 2, n)
    prv = lax.rem(me + n - 2, n)

    def cols(h):
        start = h * D
        if not isinstance(h, int):
            start = pl.multiple_of(start, D)
        return pl.ds(start, D)

    def load(i, src, dst, h):
        return pltpu.make_async_copy(
            src.at[:, cols(h)], dst.at[:, cols(h)], in_sem.at[i, h]
        )

    gate_copy = pltpu.make_async_copy(gate_hbm, gate, gate_sem.at[0])
    gate_copy.start()
    for i, (src, dst) in enumerate(((k_hbm, k), (v_hbm, v), (q_hbm, q), (g_hbm, g))):
        for h in range(H):
            load(i, src, dst, h).start()

    barrier = pltpu.get_barrier_semaphore()
    for s in (peer, nxt, prv):
        pl.semaphore_signal(barrier, inc=1, device_id={"seq": s}, device_id_type=MESH)
    for d in range(1, nh):
        pl.semaphore_signal(
            barrier, inc=1, device_id={"head": lax.rem(hd + d, nh)}, device_id_type=MESH
        )

    def remote(src, dst, s_sem, r_sem, **to):
        return pltpu.make_async_remote_copy(
            src_ref=src, dst_ref=dst, send_sem=s_sem, recv_sem=r_sem,
            device_id=to, device_id_type=MESH,
        )

    gate_copy.wait()
    l = jnp.concatenate([gate[h:h + 1, :] * -rates[h] for h in range(H)], axis=0)
    for i in range(128 // H):
        lrep[i * H:(i + 1) * H, :] = l
    ri = lax.broadcasted_iota(jnp.int32, (C, C), 0)
    ci = lax.broadcasted_iota(jnp.int32, (C, C), 1)
    triu = jnp.where(ri <= ci, 1.0, 0.0).astype(BF16)
    tot = [None] * H
    for j in range(J):
        lj = lrep[:, j * C:(j + 1) * C]
        hi = lj.astype(BF16)
        rest = lj - hi.astype(F32)
        mid = rest.astype(BF16)
        low = (rest - mid.astype(F32)).astype(BF16)
        r = dot(low, triu, 1, 0) + dot(mid, triu, 1, 0) + dot(hi, triu, 1, 0)
        brow[j] = r[0:8, :]
        col = r.T
        for h in range(H):
            b = jnp.broadcast_to(col[:, h:h + 1], (C, D))
            bc[h, j * C:(j + 1) * C, :] = b
            e = b[C - 1:C, :]
            tot[h] = e if tot[h] is None else tot[h] + e
    for h in range(H):
        gown[h:h + 1, :] = tot[h]

    gown[H:8, :] = jnp.zeros((8 - H, D), F32)
    pl.semaphore_wait(barrier, 3 + nh - 1)
    gcopy = remote(gown, gpeer, g_sem.at[0], g_sem.at[1], seq=peer)
    gcopy.start()

    def ucopy(h):
        return remote(ubuf.at[h], upeer.at[h], us.at[h], ur.at[h], seq=peer)

    half_rows = D // 2
    pieces = tuple(slice(p * half_rows, (p + 1) * half_rows) for p in range(2))

    def ccopy(h, p):
        part = pl.ds(p * half_rows, half_rows)
        return remote(cout.at[h, part], cin.at[h, part], cs.at[h, p], cr.at[h, p], seq=nxt)

    def vcopy(h):
        return remote(vbuf.at[h], vpeer.at[h], vs.at[h], vr.at[h], seq=peer)

    def dcopy(h, p):
        part = pl.ds(p * half_rows, half_rows)
        return remote(dout.at[h, part], din.at[h, part], ds.at[h, p], dr.at[h, p], seq=prv)

    def loop(lo, hi, fn):
        def step(h, carry):
            fn(h)
            return carry
        lax.fori_loop(lo, hi, step, 0)

    def rows(j):
        return slice(j * C, (j + 1) * C)

    def updates(h):
        load(0, k_hbm, k, h).wait()
        load(1, v_hbm, v, h).wait()
        s = jnp.zeros((D, D), F32)
        for j in range(J):
            b = bc[h, rows(j), :]
            e = b[C - 1:C, :]
            kd = (k[rows(j), cols(h)].astype(F32) * jnp.exp(e - b)).astype(BF16)
            u = dot(kd, v[rows(j), cols(h)], 0, 0)
            sl[h * (J + 1) + j] = s
            s = u if j == 0 else jnp.exp(e) * s + u
        sl[h * (J + 1) + J] = s
        ubuf[h] = s.astype(BF16)
        ucopy(h).start()

    loop(0, H, updates)

    def factor(h, j):
        b = bc[h, rows(j), :]
        left = jnp.concatenate([b] * (C // D), axis=1)
        right = brow[j, pl.ds(h, 1), :]
        return jnp.exp(jnp.where(ri >= ci, left - right, -jnp.inf))

    def intra(h):
        load(2, q_hbm, q, h).wait()
        for j in range(J):
            wj = dot(q[rows(j), cols(h)], k[rows(j), cols(h)], 1, 1) * factor(h, j)
            wj = wj.astype(BF16)
            w[h * J + j] = wj
            o[rows(j), cols(h)] = dot(wj, v[rows(j), cols(h)], 1, 0)

    half = H // 2
    loop(0, half, intra)
    gcopy.wait()

    def ex(ref, h):
        return jnp.exp(ref[pl.ds(h, 1), :])

    def pair(h):
        ucopy(h).wait_recv()
        own = sl[h * (J + 1) + J]

        @pl.when(inner == 0)
        def _():
            sp[h] = ex(gpeer, h) * own + upeer[h].astype(F32)

        @pl.when(inner == 1)
        def _():
            sp[h] = ex(gown, h) * upeer[h].astype(F32) + own

        @pl.when(z == 0)
        def _():
            cout[h] = sp[h].astype(BF16)
            cin[h] = jnp.zeros((D, D), BF16)

            @pl.when(z < LAST)
            def _():
                for p in range(2):
                    ccopy(h, p).start()

    loop(0, H, pair)
    loop(half, H, intra)
    for h in range(H):
        load(3, g_hbm, g, h).wait()

    def chain(h):
        @pl.when(z > 0)
        def _():
            for p, part in enumerate(pieces):
                ccopy(h, p).wait_recv()

                @pl.when(z < LAST)
                def _():
                    a = ex(gown, h) * ex(gpeer, h)
                    cout[h, part, :] = (
                        a * cin[h, part, :].astype(F32) + sp[h, part, :]
                    ).astype(BF16)
                    ccopy(h, p).start()

        @pl.when(inner == 0)
        def _():
            pstate[h] = cin[h].astype(F32)

        @pl.when(inner == 1)
        def _():
            pstate[h] = ex(gpeer, h) * cin[h].astype(F32) + upeer[h].astype(F32)

        s = pstate[h]
        for j in range(J):
            pj = (s + sl[h * (J + 1) + j] if j else s).astype(BF16)
            pchunk[h * J + j] = pj
            b = bc[h, rows(j), :]
            s = s * jnp.exp(b[C - 1:C, :])
            qe = (q[rows(j), cols(h)].astype(F32) * jnp.exp(b)).astype(BF16)
            oj = o[rows(j), cols(h)] + dot(qe, pj, 1, 0)
            o[rows(j), cols(h)] = oj
            gj = g[rows(j), cols(h)].astype(F32)

            @pl.when(h == 0)
            def _():
                macc[rows(j), :] = oj * oj
                xacc[rows(j), :] = gj * oj

            @pl.when(h > 0)
            def _():
                macc[rows(j), :] += oj * oj
                xacc[rows(j), :] += gj * oj

    loop(0, H, chain)

    NG = T // 128
    lane = lax.broadcasted_iota(jnp.int32, (128, 128), 1)
    acc = jnp.zeros((128, 128), F32)
    for u in range(NG):
        part = slice(u * 128, (u + 1) * 128)
        acc = jnp.where(lane == u, jnp.sum(macc[part, :], axis=1, keepdims=True), acc)
        acc = jnp.where(lane == NG + u, jnp.sum(xacc[part, :], axis=1, keepdims=True), acc)
    stat[...] = acc.T[0:2 * NG, :]
    scopies = [
        remote(stat, statin.at[d - 1], ss.at[d - 1], sr.at[d - 1], head=lax.rem(hd + d, nh))
        for d in range(1, nh)
    ]
    for c in scopies:
        c.start()
    for c in scopies:
        c.wait_recv()
    whole = stat[...]
    for d in range(nh - 1):
        whole = whole + statin[d]
    width = float(H * nh * D)
    root = jnp.sqrt(whole[0:NG] / width + EPS)
    tr[...] = jnp.zeros_like(tr)
    tr[0:NG, :] = 1.0 / root
    tr[NG:2 * NG, :] = whole[NG:2 * NG] / (width * root * root * root)
    back = tr[...].T
    for u in range(NG):
        part = slice(u * 128, (u + 1) * 128)
        macc[part, :] = jnp.broadcast_to(back[:, u:u + 1], (128, D))
        xacc[part, :] = jnp.broadcast_to(back[:, NG + u:NG + u + 1], (128, D))

    def outgrad(h):
        s = None
        for j in reversed(range(J)):
            do = (
                g[rows(j), cols(h)].astype(F32) * macc[rows(j), :]
                - o[rows(j), cols(h)] * xacc[rows(j), :]
            ).astype(BF16)
            dob[rows(j), cols(h)] = do
            b = bc[h, rows(j), :]
            qe = (q[rows(j), cols(h)].astype(F32) * jnp.exp(b)).astype(BF16)
            u = dot(qe, do, 0, 0)
            rl[h * (J + 1) + j + 1] = jnp.zeros((D, D), F32) if s is None else s
            s = u if s is None else u + jnp.exp(b[C - 1:C, :]) * s
        rl[h * (J + 1)] = s
        vbuf[h] = s.astype(BF16)
        vcopy(h).start()

    loop(0, H, outgrad)

    def grads(h):
        for j in range(J):
            do = dob[rows(j), cols(h)]
            e = (dot(do, v[rows(j), cols(h)], 1, 1) * factor(h, j)).astype(BF16)
            eb = jnp.exp(bc[h, rows(j), :])
            dq_out[rows(j), cols(h)] = (
                eb * dot(do, pchunk[h * J + j], 1, 1) + dot(e, k[rows(j), cols(h)], 1, 0)
            ).astype(BF16)
            dk1[rows(j), cols(h)] = dot(e, q[rows(j), cols(h)], 0, 0)
            dv1[rows(j), cols(h)] = dot(w[h * J + j], do, 0, 0)

    loop(0, half, grads)

    def pair_back(h):
        vcopy(h).wait_recv()
        own = rl[h * (J + 1)]

        @pl.when(inner == 0)
        def _():
            sp[h] = own + ex(gown, h) * vpeer[h].astype(F32)

        @pl.when(inner == 1)
        def _():
            sp[h] = vpeer[h].astype(F32) + ex(gpeer, h) * own

        @pl.when(z == LAST)
        def _():
            dout[h] = sp[h].astype(BF16)
            din[h] = jnp.zeros((D, D), BF16)

            @pl.when(z > 0)
            def _():
                for p in range(2):
                    dcopy(h, p).start()

    loop(0, H, pair_back)
    loop(half, H, grads)

    def chain_back(h):
        @pl.when(z < LAST)
        def _():
            for p, part in enumerate(pieces):
                dcopy(h, p).wait_recv()

                @pl.when(z > 0)
                def _():
                    a = ex(gown, h) * ex(gpeer, h)
                    dout[h, part, :] = (
                        a * din[h, part, :].astype(F32) + sp[h, part, :]
                    ).astype(BF16)
                    dcopy(h, p).start()

        @pl.when(inner == 1)
        def _():
            pstate[h] = din[h].astype(F32)

        @pl.when(inner == 0)
        def _():
            pstate[h] = ex(gpeer, h) * din[h].astype(F32) + vpeer[h].astype(F32)

        s = pstate[h]
        for j in reversed(range(J)):
            rj = (s + rl[h * (J + 1) + j + 1] if j < J - 1 else s).astype(BF16)
            b = bc[h, rows(j), :]
            e = b[C - 1:C, :]
            s = s * jnp.exp(e)
            tail = jnp.exp(e - b)
            dk_out[rows(j), cols(h)] = (
                dk1[rows(j), cols(h)] + tail * dot(v[rows(j), cols(h)], rj, 1, 1)
            ).astype(BF16)
            dv_out[rows(j), cols(h)] = (
                dv1[rows(j), cols(h)] + tail * dot(k[rows(j), cols(h)], rj, 1, 0)
            ).astype(BF16)

    loop(0, H, chain_back)

    for c in scopies:
        c.wait_send()

    def drain(h):
        ucopy(h).wait_send()
        vcopy(h).wait_send()

        @pl.when(z < LAST)
        def _():
            for p in range(2):
                ccopy(h, p).wait_send()

        @pl.when(z > 0)
        def _():
            for p in range(2):
                dcopy(h, p).wait_send()

    loop(0, H, drain)


def body(queries, key_vectors, value_vectors, out_grad, head_rates, gate_scale):
    H, T = gate_scale.shape
    D = queries.shape[1] // H
    n = lax.axis_size("seq")
    nh = lax.axis_size("head")
    C = min(256, T)
    J = T // C
    tile = pltpu.VMEM((H, D, D), BF16)
    full = pltpu.VMEM((T, H * D), BF16)
    wide = pltpu.VMEM((T, H * D), F32)
    sem = pltpu.SemaphoreType.DMA
    out = pltpu.VMEM((T, H * D), BF16)
    vm = pl.BlockSpec(memory_space=pltpu.VMEM)
    hbm = pl.BlockSpec(memory_space=pl.ANY)
    return pl.pallas_call(
        functools.partial(kernel, n, nh, H, T, D, C),
        out_shape=(out, out, out),
        in_specs=[pl.BlockSpec(memory_space=pltpu.SMEM), hbm, hbm, hbm, hbm, hbm],
        out_specs=(vm, vm, vm),
        scratch_shapes=[
            pltpu.VMEM((H, T), F32),
            full, full, full, full,
            pltpu.VMEM((128, T), F32),
            pltpu.VMEM((J, 8, C), F32),
            pltpu.VMEM((H, T, D), F32),
            pltpu.VMEM((8, D), F32),
            pltpu.VMEM((8, D), F32),
            pltpu.VMEM((H * (J + 1), D, D), F32),
            pltpu.VMEM((H * J, C, C), BF16),
            wide,
            pltpu.VMEM((T, D), F32),
            pltpu.VMEM((T, D), F32),
            pltpu.VMEM((H, D, D), F32),
            pltpu.VMEM((H * J, D, D), BF16),
            pltpu.VMEM((H, D, D), F32),
            tile, tile, tile, tile,
            pltpu.VMEM((2 * T // 128, 128), F32),
            pltpu.VMEM((nh - 1, 2 * T // 128, 128), F32),
            pltpu.VMEM((128, 128), F32),
            full,
            tile, tile, tile, tile,
            pltpu.VMEM((H * (J + 1), D, D), F32),
            wide, wide,
            sem((4, H)), sem((1,)), sem((2,)),
            sem((H,)), sem((H,)), sem((H, 2)), sem((H, 2)),
            sem((nh - 1,)), sem((nh - 1,)),
            sem((H,)), sem((H,)), sem((H, 2)), sem((H, 2)),
        ],
        compiler_params=pltpu.CompilerParams(
            collective_id=0, has_side_effects=True, vmem_limit_bytes=63692800
        ),
    )(head_rates, gate_scale, queries, key_vectors, value_vectors, out_grad)


def solution(mesh):
    placed = (
        P("seq", "head"),
        P("seq", "head"),
        P("seq", "head"),
        P("seq", "head"),
        P("head"),
        P("head", "seq"),
    )
    return jax.shard_map(
        body,
        mesh=mesh,
        in_specs=placed,
        out_specs=(P("seq", "head"), P("seq", "head"), P("seq", "head")),
        check_vma=False,
    )
```
